32 devices in a mesh: groups: 2 (over y), ep: 4 (over z), dp: 4 (over x, core), tp: 1.
Axes of the slice: x: 2, y: 2, z: 4, core: 2. Of those that a mesh axis runs over, the one named last changes fastest.
Arguments:
- tokens: bfloat16 [2048, 2048], P(('groups', 'ep', 'dp', 'tp')), parts along dimension 0, may hold values from -6 to 6
- experts_one: int32 [2048, 8], P(('groups', 'ep', 'dp', 'tp')), parts along dimension 0, may hold values from 0 to 15, all different within a row; in each aligned block of 64 rows (0 to 63, 64 to 127, ...) at most 40 rows name the same one
- gates_one: float32 [2048, 8], P(('groups', 'ep', 'dp', 'tp')), parts along dimension 0, may hold values from 0.05 to 0.5
- w_in_one: bfloat16 [16, 2048, 2, 768], P(('ep', 'dp'), None, None, 'tp'), may hold values from -0.125 to 0.125
- w_down_one: bfloat16 [16, 768, 2048], P(('ep', 'dp'), 'tp'), may hold values from -0.21875 to 0.21875
- norm_gain: float32 [2048], replicated, may hold values from 0.5 to 1.5
- experts_two: int32 [2048, 8], P(('groups', 'ep', 'dp', 'tp')), parts along dimension 0, may hold values from 0 to 15, all different within a row; in each aligned block of 64 rows (0 to 63, 64 to 127, ...) at most 40 rows name the same one
- gates_two: float32 [2048, 8], P(('groups', 'ep', 'dp', 'tp')), parts along dimension 0, may hold values from 0.05 to 0.5
- placement_two: int32 [16], replicated, may hold values from 0 to 15, each once
- w_in_two: bfloat16 [16, 2048, 2, 768], P(('ep', 'dp'), None, None, 'tp'), may hold values from -0.125 to 0.125
- w_down_two: bfloat16 [16, 768, 2048], P(('ep', 'dp'), 'tp'), may hold values from -0.21875 to 0.21875
Outputs:
- layer_out: bfloat16 [2048, 2048], P(('groups', 'ep', 'dp', 'tp')), parts along dimension 0
The draws below stay inside these ranges and needn't reach their ends.
There are 2 independent parts, one for each index of `groups`. The reference program is written for one: setup_inputs(seed, part) draws one part's arguments, and reference() takes and returns one part's arrays. A program takes and returns all parts, laid end to end along the dimension named above; an argument that names none is the same for every part. Nothing has to cross between parts.
Inputs may be any that keep to these rules, and one draw needn't show every extreme that they name: `experts_one`: each token names 8 different experts; among the 64 tokens of one device no expert is named more than 40 times, and on some device some expert is named exactly 40 times. `experts_two`: each token names 8 different experts; among the 64 tokens of one device no expert is named more than 40 times, and on some device some expert is named exactly 40 times. `placement_two`: each slot is named by exactly one expert.
All inputs are finite; a program needn't handle non-finite values.
Results may differ from the reference program's by a relative error of at most 0.011.
Values may be sent and summed in bfloat16 or wider, within the bound.
No kernel may reach another device: no remote copies, remote signals or barrier semaphores. Data moves between devices by JAX's collectives and lax.ppermute only.
A program may use at most 128 MiB of HBM per device.

```python
import math
import jax
import jax.numpy as jnp
import numpy as np
from jax import lax

D = 2048
FF = 768
TOPK = 8
TOK_DEV = 64
EXPERTS = 16
MOST = 40
TOKENS = 1024
N_EP = 4
N_DP = 4
N_TP = 1


def shard_levels(key, dims, cuts, smallest, top_value):
    loudness, own = 1.0, jax.random.fold_in(key, 6)
    for position, parts in cuts:
        heights = jnp.exp(jax.random.uniform(jax.random.fold_in(own, position), (parts,), jnp.float32, smallest / len(cuts), top_value / len(cuts)))
        loudness = loudness * jnp.repeat(heights, dims[position] // parts).reshape([-1 if axis == position else 1 for axis in range(len(dims))])
    return loudness


def assign_block(stream_key, own, number, rows, count, top, limit, lean):
    sequence = jax.random.permutation(stream_key, count)
    crowded, common = shares(count, rows * top, limit, lean, True), shares(count, rows * top, limit, lean, False)
    places = jnp.arange(count)

    def named(sizes, rotation):
        used = int((sizes > 0).sum())
        fixed = max(1, used // 4)
        passed = fixed + (places - fixed + rotation * (used - fixed)) % max(1, count - fixed)
        return jnp.zeros((count,), jnp.int32).at[sequence[jnp.where(places < fixed, places, passed)]].set(jnp.asarray(sizes, jnp.int32))

    sizes = jnp.where(number % 4 == 0, named(crowded, number // 4), named(common, number - number // 4 - 1))
    mixed = jax.random.permutation(jax.random.fold_in(own, 3), count)
    giver, receiver = mixed[0:count // 2 * 2:2], mixed[1:count // 2 * 2:2]
    margin = jnp.minimum(sizes[giver] - 1, limit - sizes[receiver]) // 2
    margin = jnp.where((giver == sequence[0]) | (receiver == sequence[0]) | (sizes[receiver] == 0), 0, jnp.maximum(margin, 0))
    passed = jax.random.randint(jax.random.fold_in(own, 4), (count // 2,), 0, 1 << 20) % (margin + 1)
    sizes = sizes.at[giver].add(-passed).at[receiver].add(passed)
    labels = jnp.searchsorted(jnp.cumsum(sizes), jnp.arange(rows * top), side="right").astype(jnp.int32)
    listing = labels.reshape(top, rows).T
    listing = listing[jax.random.permutation(jax.random.fold_in(own, 1), rows)]
    rotation = jax.random.randint(jax.random.fold_in(own, 2), (rows, 1), 0, top)
    return jnp.take_along_axis(listing, (jnp.arange(top)[None, :] + rotation) % top, axis=1)


def shares(count, total, bound, lean, full):
    weights = [(1 << 20) // math.isqrt(rank ** lean) + 1 for rank in range(1, count + 1)]
    largest = bound if full else min(bound, max(-(-total // count), total * weights[0] // sum(weights)))
    least = 1 if total - largest >= count - 1 else 0
    holding, spare = [largest] + [least] * (count - 1), total - largest - least * (count - 1)
    while spare > 0:
        candidates = [i for i in range(1, count) if holding[i] < largest] or [i for i in range(1, count) if holding[i] < bound]
        whole, remaining = sum([weights[i] for i in candidates]), spare
        for i in candidates:
            more = min(bound - holding[i], max(1, remaining * weights[i] // whole), spare)
            holding[i] = holding[i] + more
            spare = spare - more
    return np.array(holding)


def gaussian(own_key, extent, scale, reach, cuts=(), kind=jnp.bfloat16):
    entries = jax.random.normal(own_key, extent, jnp.float32) * scale
    if len(cuts) > 0:
        entries = shard_levels(own_key, extent, cuts, -0.22, 0.18) * entries
    return jnp.clip(entries, min=-reach, max=reach).astype(kind)


def setup_inputs(seed: int = 0, part: int = 0) -> dict:
    key_of = jax.random.split(jax.random.key(seed), 12)
    part_splits = jax.random.split(jax.random.fold_in(key_of[11], part), 12)
    tokens = gaussian(part_splits[0], (TOKENS, D), 1.0, 6.0, ((0, 16),))
    experts_one_keys = jax.random.split(jax.random.fold_in(part_splits[1], 1), TOKENS // TOK_DEV)
    experts_one_turns = jax.random.permutation(jax.random.fold_in(part_splits[1], 3), TOKENS // TOK_DEV)
    experts_one = jax.vmap(lambda own, number: assign_block(jax.random.fold_in(part_splits[1], 2), own, number, TOK_DEV, EXPERTS, TOPK, MOST, 2))(experts_one_keys, experts_one_turns).reshape((TOKENS, TOPK))
    gates_one = jnp.clip(jnp.exp(math.log(0.5) - 2.3025851 * jax.random.uniform(part_splits[2], (TOKENS, TOPK), jnp.float32) ** shard_levels(part_splits[2], (TOKENS, TOPK), ((0, 16),), -0.2, 0.2)), 0.05, 0.5)
    w_in_one = gaussian(key_of[3], (EXPERTS, D, 2, FF), D ** -0.5, 0.125, ((0, 16),))
    w_down_one = gaussian(key_of[4], (EXPERTS, FF, D), FF ** -0.5, 0.21875, ((0, 16),))
    norm_gain = jnp.clip(1.0 + 0.1 * jax.random.normal(key_of[5], (D,), jnp.float32), 0.5, 1.5)
    experts_two_keys = jax.random.split(jax.random.fold_in(part_splits[6], 1), TOKENS // TOK_DEV)
    experts_two_turns = jax.random.permutation(jax.random.fold_in(part_splits[6], 3), TOKENS // TOK_DEV)
    experts_two = jax.vmap(lambda own, number: assign_block(jax.random.fold_in(part_splits[6], 2), own, number, TOK_DEV, EXPERTS, TOPK, MOST, 2))(experts_two_keys, experts_two_turns).reshape((TOKENS, TOPK))
    gates_two = jnp.clip(jnp.exp(math.log(0.5) - 2.3025851 * jax.random.uniform(part_splits[7], (TOKENS, TOPK), jnp.float32) ** shard_levels(part_splits[7], (TOKENS, TOPK), ((0, 16),), -0.2, 0.2)), 0.05, 0.5)
    placement_two = jax.random.permutation(key_of[8], EXPERTS).astype(jnp.int32)
    w_in_two = gaussian(key_of[9], (EXPERTS, D, 2, FF), D ** -0.5, 0.125, ((0, 16),))
    w_down_two = gaussian(key_of[10], (EXPERTS, FF, D), FF ** -0.5, 0.21875, ((0, 16),))
    return dict(tokens=tokens, experts_one=experts_one, gates_one=gates_one, w_in_one=w_in_one, w_down_one=w_down_one, norm_gain=norm_gain, experts_two=experts_two, gates_two=gates_two, placement_two=placement_two, w_in_two=w_in_two, w_down_two=w_down_two)


def expert_layer(rows_in, layer_slots, gate_values, w_in, w_down):
    token_count, top_count = layer_slots.shape
    expert_total, row_width, pair_n, hidden_n = w_in.shape
    slot_cap = MOST * N_EP * N_DP * N_TP
    block_width = hidden_n // N_TP
    flat_ids = layer_slots.reshape(-1)
    owner_row = jnp.arange(token_count * top_count, dtype=jnp.int32) // top_count
    flat_gates = gate_values.reshape(-1)

    def accumulate(summed, expert_id):
        hit_mask = flat_ids == expert_id
        slot_rank = jnp.cumsum(hit_mask.astype(jnp.int32)) - 1
        slot_pos = jnp.where(hit_mask, slot_rank, slot_cap).astype(jnp.int32)
        picked = jnp.zeros((slot_cap,), jnp.int32).at[slot_pos].set(owner_row, mode='drop')
        weight = jnp.zeros((slot_cap,), jnp.float32).at[slot_pos].set(flat_gates, mode='drop')
        chosen = rows_in[picked]
        gate_up = jnp.dot(chosen, w_in[expert_id].reshape(row_width, pair_n * hidden_n), preferred_element_type=jnp.float32)
        activated = (jax.nn.silu(gate_up[:, :hidden_n]) * gate_up[:, hidden_n:]).astype(jnp.bfloat16)
        down_now = w_down[expert_id]
        total = jnp.zeros((slot_cap, row_width), jnp.float32)
        for block in range(N_TP):
            lo_unit = block * block_width
            partial_out = jnp.dot(activated[:, lo_unit:lo_unit + block_width], down_now[lo_unit:lo_unit + block_width], preferred_element_type=jnp.float32)
            total = total + partial_out.astype(jnp.bfloat16).astype(jnp.float32)
        expert_out = total.astype(jnp.bfloat16)
        summed = summed.at[picked].add(weight[:, None] * expert_out.astype(jnp.float32))
        return (summed, None)
    start_sum = jnp.zeros((token_count, row_width), jnp.float32)
    summed, _ = lax.scan(accumulate, start_sum, jnp.arange(expert_total, dtype=jnp.int32))
    return summed

def reference(tokens, experts_one, gates_one, w_in_one, w_down_one, norm_gain, experts_two, gates_two, placement_two, w_in_two, w_down_two):
    moe_one = expert_layer(tokens, experts_one, gates_one, w_in_one, w_down_one)
    mixed = (tokens.astype(jnp.float32) + moe_one).astype(jnp.bfloat16)
    mixed = lax.optimization_barrier(mixed)
    mixed_wide = mixed.astype(jnp.float32)
    inv_rms = lax.rsqrt(lax.optimization_barrier(jnp.mean(mixed_wide * mixed_wide, axis=1, keepdims=True)) + 1e-06)
    normed = (mixed_wide * inv_rms * norm_gain[None, :]).astype(jnp.bfloat16)
    layer_slots = placement_two[experts_two].astype(jnp.int32)
    moe_two = expert_layer(normed, layer_slots, gates_two, w_in_two, w_down_two)
    return (mixed_wide + moe_two).astype(jnp.bfloat16)
```

```python
import functools

import jax
import jax.numpy as jnp
from jax import lax
from jax.experimental import pallas as pl
from jax.experimental.pallas import tpu as pltpu
from jax.sharding import PartitionSpec as P

LANES = 128


def capacity(tok_rows, top_count, expert_count):
    return max(2, min(tok_rows, 5 * tok_rows * top_count // (4 * expert_count)))


def pack_rows(rows_in, targets, expert_count, per_slot):
    tok_rows, top_count = targets.shape
    flat_ids = targets.reshape(-1)
    hit_table = (flat_ids[:, None] == jnp.arange(expert_count, dtype=jnp.int32)[None, :]).astype(
        jnp.int32
    )
    before = jnp.cumsum(hit_table, axis=0) - hit_table
    slot_rank = jnp.sum(before * hit_table, axis=1)
    slot_index = flat_ids * per_slot + slot_rank
    source = jnp.arange(tok_rows * top_count, dtype=jnp.int32) // top_count
    owner_row = jnp.zeros((expert_count * per_slot,), jnp.int32).at[slot_index].set(source)
    filled = jnp.zeros((expert_count * per_slot,), jnp.int32).at[slot_index].set(1)
    buffer = jnp.where(filled[:, None] > 0, rows_in[owner_row], jnp.zeros((), rows_in.dtype))
    return (buffer, slot_index)


def exchange(buffer, expert_count, per_slot):
    row_width = buffer.shape[1]
    moved = lax.all_to_all(
        buffer.reshape(expert_count, per_slot, row_width),
        ("ep", "dp"),
        split_axis=0,
        concat_axis=0,
        tiled=True,
    )
    return moved.reshape(expert_count * per_slot, row_width)


def run_expert(received, w_in, w_down):
    row_width = received.shape[1]
    down_local = w_down[0]
    half_width = down_local.shape[0]
    w_local = w_in.reshape(row_width, 2 * half_width)
    gate_up = jnp.dot(
        lax.all_gather(received, "tp", axis=0, tiled=True),
        w_local,
        preferred_element_type=jnp.float32,
    )
    hidden = (jax.nn.silu(gate_up[:, :half_width]) * gate_up[:, half_width:]).astype(jnp.bfloat16)
    return lax.psum_scatter(
        jnp.dot(hidden, down_local, preferred_element_type=jnp.float32).astype(jnp.bfloat16),
        "tp",
        scatter_dimension=0,
        tiled=True,
    )


def moe_block(rows_in, targets, gate_values, w_in, w_down, expert_count, per_slot):
    tok_rows, top_count = targets.shape
    row_width = rows_in.shape[1]
    buffer, slot_index = pack_rows(rows_in, targets, expert_count, per_slot)
    arrived = exchange(buffer, expert_count, per_slot)
    produced = run_expert(arrived, w_in, w_down)
    returned = exchange(produced, expert_count, per_slot)
    picked = returned[slot_index].reshape(tok_rows, top_count, row_width)
    return jnp.sum(gate_values[:, :, None] * picked.astype(jnp.float32), axis=1)


def slots_of(experts_two, placement_two):
    expert_range = jnp.arange(placement_two.shape[0], dtype=jnp.int32)
    matches = experts_two[:, :, None] == expert_range[None, None, :]
    return jnp.sum(jnp.where(matches, placement_two[None, None, :], 0), axis=2)


def norm_rows(mixed, norm_gain):
    mixed_wide = mixed.astype(jnp.float32)
    inv_rms = lax.rsqrt(jnp.mean(mixed_wide * mixed_wide, axis=1, keepdims=True) + 1e-06)
    return (mixed_wide * inv_rms * norm_gain[None, :]).astype(jnp.bfloat16)


def routed_shards(
    tokens,
    experts_one,
    gates_one,
    w_in_one,
    w_down_one,
    norm_gain,
    experts_two,
    gates_two,
    placement_two,
    w_in_two,
    w_down_two,
):
    tok_rows, top_count = experts_one.shape
    expert_count = placement_two.shape[0]
    per_slot = capacity(tok_rows, top_count, expert_count)
    moe_one = moe_block(
        tokens, experts_one, gates_one, w_in_one, w_down_one, expert_count, per_slot
    )
    mixed = (tokens.astype(jnp.float32) + moe_one).astype(jnp.bfloat16)
    mixed = lax.optimization_barrier(mixed)
    normed = norm_rows(mixed, norm_gain)
    layer_slots = slots_of(experts_two, placement_two)
    moe_two = moe_block(
        normed, layer_slots, gates_two, w_in_two, w_down_two, expert_count, per_slot
    )
    return (mixed.astype(jnp.float32) + moe_two).astype(jnp.bfloat16)


def gate_columns(targets, gate_values, expert_count):
    hits = targets[:, :, None] == jnp.arange(expert_count, dtype=jnp.int32)[None, None, :]
    table = jnp.sum(jnp.where(hits, gate_values[:, :, None], 0.0), axis=1)
    high = lax.reduce_precision(table, 8, 7)
    rest = table - high
    middle = lax.reduce_precision(rest, 8, 7)
    low = rest - middle
    return jnp.concatenate([high, middle, low], axis=1).astype(jnp.bfloat16)


def mlp_kernel(block_count, rows, width, half, lane_base, expert_count, chunk, *refs):
    ids = refs[0]
    x_in = refs[1 : 1 + block_count]
    g_in = refs[1 + block_count : 1 + 2 * block_count]
    weights = refs[1 + 2 * block_count : 5 + 2 * block_count]
    outs = refs[5 + 2 * block_count : 5 + 3 * block_count]
    xs, gs, w_in, w_down, hidden, total, x_sem, g_sem, in_sem, down_sem = refs[
        5 + 3 * block_count :
    ]
    pieces = half // chunk

    x_copies, g_copies = [], []
    for k in range(block_count):
        span = pl.ds(k * rows, rows)
        x_copies.append(
            pltpu.make_async_copy(x_in[k].at[:, pl.ds(0, width)], xs.at[span, :], x_sem.at[k])
        )
        g_copies.append(
            pltpu.make_async_copy(
                g_in[k].at[:, pl.ds(width, LANES)], gs.at[span, :], g_sem.at[k]
            )
        )
    for copy in x_copies:
        copy.start()
    in_copies, down_copies = {}, {}
    for e in range(2):
        for j in range(pieces):
            for part in range(2):
                cols = pl.ds(part * half + j * chunk, chunk)
                copy = pltpu.make_async_copy(
                    weights[2 * e].at[:, cols],
                    w_in.at[e, part, j],
                    in_sem.at[e, part, j],
                )
                copy.start()
                in_copies[e, part, j] = copy
        down_copies[e] = pltpu.make_async_copy(weights[2 * e + 1], w_down.at[e], down_sem.at[e])
        down_copies[e].start()
        if e == 0:
            for copy in g_copies:
                copy.start()
    for copy in x_copies:
        copy.wait()
    for e in range(2):
        for j in range(pieces):
            in_copies[e, 0, j].wait()
            in_copies[e, 1, j].wait()
            gate = jnp.dot(xs[...], w_in[e, 0, j], preferred_element_type=jnp.float32)
            up = jnp.dot(xs[...], w_in[e, 1, j], preferred_element_type=jnp.float32)
            act = gate / (1.0 + jnp.exp(-gate)) * up
            hidden[:, j * chunk : (j + 1) * chunk] = act.astype(jnp.bfloat16)
        down_copies[e].wait()
        if e == 0:
            for copy in g_copies:
                copy.wait()
        lane = lax.broadcasted_iota(jnp.int32, gs.shape, 1) - lane_base - ids[e]
        mine = (lane == 0) | (lane == expert_count) | (lane == 2 * expert_count)
        scale = jnp.sum(
            jnp.where(mine, gs[...].astype(jnp.float32), 0.0), axis=1, keepdims=True
        )
        for n in range(width // 512):
            cols = slice(n * 512, (n + 1) * 512)
            piece = scale * jnp.dot(
                hidden[...], w_down[e, :, cols], preferred_element_type=jnp.float32
            )
            if e == 0:
                total[:, cols] = piece
            else:
                piece = (total[:, cols] + piece).astype(jnp.bfloat16)
                for k in range(block_count):
                    outs[k][:, cols] = piece[k * rows : (k + 1) * rows]


def mlp_blocks(blocks, gate_blocks, weights, ids, lane_base, expert_count, width):
    block_count = len(blocks)
    rows = blocks[0].shape[0]
    half = weights[1].shape[0]
    chunk = 256 if half % 256 == 0 else half
    all_rows = block_count * rows
    anywhere = pl.BlockSpec(memory_space=pl.ANY)
    return pl.pallas_call(
        functools.partial(
            mlp_kernel, block_count, rows, width, half, lane_base, expert_count, chunk
        ),
        out_shape=[jax.ShapeDtypeStruct((rows, width), jnp.bfloat16)] * block_count,
        in_specs=[pl.BlockSpec(memory_space=pltpu.SMEM)]
        + [anywhere] * (2 * block_count + 4),
        out_specs=[pl.BlockSpec(memory_space=pltpu.VMEM)] * block_count,
        scratch_shapes=[
            pltpu.VMEM((all_rows, width), jnp.bfloat16),
            pltpu.VMEM((all_rows, LANES), jnp.bfloat16),
            pltpu.VMEM((2, 2, half // chunk, width, chunk), jnp.bfloat16),
            pltpu.VMEM((2, half, width), jnp.bfloat16),
            pltpu.VMEM((all_rows, half), jnp.bfloat16),
            pltpu.VMEM((all_rows, width), jnp.float32),
            pltpu.SemaphoreType.DMA((block_count,)),
            pltpu.SemaphoreType.DMA((block_count,)),
            pltpu.SemaphoreType.DMA((2, 2, half // chunk)),
            pltpu.SemaphoreType.DMA((2,)),
        ],
        compiler_params=pltpu.CompilerParams(vmem_limit_bytes=48 * 1024 * 1024),
        cost_estimate=pl.CostEstimate(
            flops=12 * all_rows * width * half,
            bytes_accessed=12 * width * half,
            transcendentals=2 * all_rows * half,
        ),
        name="expert_pair",
    )(ids, *blocks, *gate_blocks, *weights)


def multicast_shards(
    ep_count,
    chips,
    tokens,
    experts_one,
    gates_one,
    w_in_one,
    w_down_one,
    norm_gain,
    experts_two,
    gates_two,
    placement_two,
    w_in_two,
    w_down_two,
):
    rows, width = tokens.shape
    expert_count = placement_two.shape[0]
    half = w_down_one.shape[1]
    chip_count = len(chips)
    dp_count = 2 * chip_count
    twin = [(a, b) for pair in chips for a, b in (pair, pair[::-1])]

    def along_ep(array, shift):
        pairs = [(i, (i + shift) % ep_count) for i in range(ep_count)]
        return lax.ppermute(array, "ep", pairs)

    def along_chips(array, shift):
        pairs = []
        for i, pair in enumerate(chips):
            goal = chips[(i + shift) % chip_count]
            pairs += [(pair[0], goal[0]), (pair[1], goal[1])]
        return lax.ppermute(array, "dp", pairs)

    def across(array):
        return lax.ppermute(array, "dp", twin)

    def weights_of(w_in, w_down):
        flat = w_in.reshape(width, 2 * half)
        down = w_down[0]
        return (flat, down, across(flat), across(down))

    place = jnp.asarray([b for _, b in sorted(twin)], jnp.int32)
    me = lax.axis_index("dp")
    base = lax.axis_index("ep") * dp_count
    ids = jnp.stack([base + me, base + place[me]]).astype(jnp.int32)

    gates = jnp.concatenate(
        [
            gate_columns(experts_one, gates_one, expert_count),
            gate_columns(slots_of(experts_two, placement_two), gates_two, expert_count),
        ],
        axis=1,
    )
    gates = jnp.pad(gates, ((0, 0), (0, LANES - gates.shape[1])))

    def spread(block):
        mine = [block] + [along_ep(block, k) for k in range(1, ep_count)]
        others = [[along_chips(b, s) for b in mine] for s in range(1, chip_count)]
        return mine, others

    def gather_back(mine, others):
        partial = []
        for k in range(ep_count):
            value = mine[k].astype(jnp.float32)
            for s in range(1, chip_count):
                value = value + along_chips(others[s - 1][k], -s).astype(jnp.float32)
            partial.append(value)
        total = partial[0]
        for k in range(1, ep_count):
            total = total + along_ep(partial[k].astype(jnp.bfloat16), -k).astype(jnp.float32)
        return total

    def layer(block, gate_blocks, weights, lane_base):
        mine, others = spread(block)
        if gate_blocks is None:
            gate_blocks = [mine] + others
        sums = [
            mlp_blocks(bl, gb, weights, ids, lane_base, expert_count, width)
            for bl, gb in zip([mine] + others, gate_blocks)
        ]
        return gather_back(sums[0], sums[1:]), gate_blocks

    payload = jnp.concatenate([tokens, gates], axis=1)
    weights_one = weights_of(w_in_one, w_down_one)
    weights_two = weights_of(w_in_two, w_down_two)
    moe_one, gate_blocks = layer(payload, None, weights_one, 0)
    mixed = (tokens.astype(jnp.float32) + moe_one).astype(jnp.bfloat16)
    mixed = lax.optimization_barrier(mixed)
    normed = norm_rows(mixed, norm_gain)
    moe_two, _ = layer(normed, gate_blocks, weights_two, 3 * expert_count)
    return (mixed.astype(jnp.float32) + moe_two).astype(jnp.bfloat16)


def chip_pairs(mesh):
    names = mesh.axis_names
    axes = [names.index(n) for n in ("groups", "ep", "dp", "tp")]
    devices = mesh.devices.transpose(axes)
    if devices.shape[3] != 1:
        return None
    found = None
    for line in devices[..., 0].reshape(-1, devices.shape[2]):
        chips = {}
        for i, device in enumerate(line):
            chips.setdefault(tuple(getattr(device, "coords", (i,))), []).append(i)
        pairs = [tuple(v) for v in chips.values()]
        if any(len(p) != 2 for p in pairs) or found not in (None, pairs):
            return None
        found = pairs
    return found


def solution(mesh):
    in_specs = (
        P(("groups", "ep", "dp", "tp"), None),
        P(("groups", "ep", "dp", "tp"), None),
        P(("groups", "ep", "dp", "tp"), None),
        P(("ep", "dp"), None, None, "tp"),
        P(("ep", "dp"), "tp", None),
        P(),
        P(("groups", "ep", "dp", "tp"), None),
        P(("groups", "ep", "dp", "tp"), None),
        P(),
        P(("ep", "dp"), None, None, "tp"),
        P(("ep", "dp"), "tp", None),
    )
    out_specs = P(("groups", "ep", "dp", "tp"), None)
    chips = chip_pairs(mesh)

    def run(*args):
        experts, top_count = args[8].shape[0], args[1].shape[1]
        body = routed_shards
        if chips is not None and experts <= 2 * top_count and 6 * experts <= LANES:
            body = functools.partial(multicast_shards, mesh.shape["ep"], chips)
        return jax.shard_map(
            body, mesh=mesh, in_specs=in_specs, out_specs=out_specs, check_vma=False
        )(*args)

    return run
```
